32 devices in a mesh: dp: 4 (over y, x), seq: 8 (over z, core).
Axes of the slice: x: 2, y: 2, z: 4, core: 2. Of those that a mesh axis runs over, the one named last changes fastest.
Arguments:
- tokens: bfloat16 [4, 4096, 2560], P('dp', 'seq'), may hold values from -6 to 6
- w_x: bfloat16 [2560, 3072], P('seq'), may hold values from -0.125 to 0.125
- w_bc: bfloat16 [2560, 256], P('seq'), may hold values from -0.125 to 0.125
- w_dt: bfloat16 [2560, 48], P('seq'), may hold values from -0.125 to 0.125
- dt_bias: float32 [48], replicated, may hold values from -1 to 0.5
- decay_rate: float32 [48], replicated, may hold values from 9.765625e-05 to 0.12
- gain: float32 [3072], replicated, may hold values from 0.5 to 1.5
- cotangent: bfloat16 [4, 4096, 3072], P('dp', 'seq'), may hold values from -0.005859375 to 0.005859375
- counts: int32 [8], replicated, may hold values from 1 to 2, 12 in all
Outputs:
- ssm_output: bfloat16 [4, 4096, 3072], P('dp', 'seq')
- grad_c: float32 [2560, 128], P('seq')
The draws below stay inside these ranges and needn't reach their ends.
Inputs may be any that keep to these rules, and one draw needn't show every extreme that they name: counts add up to 12 and one of them equals 2.
All inputs are finite; a program needn't handle non-finite values.
Results may differ from the reference program's by a relative error of at most 0.02.
Values may be sent and summed in bfloat16 or wider, within the bound.
A program may use at most 128 MiB of HBM per device.

```python
import math
import jax
import jax.numpy as jnp
import numpy as np
from jax import lax

D = 2560
H = 48
P_SIZE = 64
N = 128
L = 256
CAP = 2
GROUPS = 8
BATCH = 4
TOTAL = 12
ROWS = 4096


def draw_decay_rate(key, part):
    key_kind = jax.random.fold_in(key, 11)
    key_slow = jax.random.fold_in(key, 12)
    key_fast = jax.random.fold_in(key, 13)
    key_middle = jax.random.fold_in(key, 14)
    slow_share = 0.4
    middle_share = 0.3
    picker = jax.random.uniform(key_kind, (H,))
    slow_rate = jnp.exp(jax.random.uniform(key_slow, (H,), minval=math.log(0.3), maxval=math.log(2.0))) / (TOTAL * L)
    middle_rate = jnp.exp(jax.random.uniform(key_middle, (H,), minval=math.log(0.0015), maxval=math.log(0.006)))
    fast_rate = jnp.exp(jax.random.uniform(key_fast, (H,), minval=math.log(0.04), maxval=math.log(0.12)))
    chosen = jnp.where(picker < slow_share, slow_rate, jnp.where(picker < slow_share + middle_share, middle_rate, fast_rate))
    return chosen.astype(jnp.float32)


def block_levels(key, dims, pieces, smallest, top_value):
    level = 1.0
    for axis_at, blocks in pieces:
        draws = jax.random.uniform(jax.random.fold_in(jax.random.fold_in(key, 6), axis_at), (blocks,), jnp.float32, smallest / len(pieces), top_value / len(pieces))
        level = level * jnp.repeat(jnp.exp(draws), dims[axis_at] // blocks).reshape((-1,) + (1,) * (len(dims) - 1 - axis_at))
    return level


def profile(amount, total, limit, skew):
    portions = [(1 << 20) // math.isqrt(standing ** skew) + 1 for standing in range(2, amount + 1)]
    spare, given = total - limit - (amount - 1), [1] * (amount - 1)
    while spare > 0:
        candidates = [i for i in range(amount - 1) if given[i] < limit]
        whole, left = sum([portions[i] for i in candidates]), spare
        for i in candidates:
            addition = min(limit - given[i], max(1, left * portions[i] // whole), spare)
            given[i] = given[i] + addition
            spare = spare - addition
    return np.array([limit] + given)


def ragged(key, number_of, total, reach, slope):
    if number_of == 2:
        one = jax.random.randint(key, (), max(1, total - reach), min(reach, total - 1) + 1)
        return jnp.stack([one, total - one])
    sizes = jnp.asarray(profile(number_of, total, reach, slope), jnp.int32)
    twos = (number_of - 1) // 2
    source_of, taker = sizes[1:1 + 2 * twos:2], sizes[2:2 + 2 * twos:2]
    slack = jnp.minimum(source_of - 1, reach - taker)
    moved = jax.random.randint(jax.random.fold_in(key, 1), (twos,), 0, 1 << 20) % (slack + 1)
    sizes = sizes.at[1:1 + 2 * twos:2].set(source_of - moved).at[2:2 + 2 * twos:2].set(taker + moved)
    return sizes[jax.random.permutation(jax.random.fold_in(key, 2), number_of)]


def scatter_about(stream_key, shape, scale, reach, split=(), dtype=jnp.bfloat16):
    level = block_levels(stream_key, shape, split, -0.22, 0.18) if split else 1.0
    drawn = jax.random.normal(stream_key, shape, jnp.float32) * scale * level
    return jnp.minimum(jnp.maximum(drawn, -reach), reach).astype(dtype)


def setup_inputs(seed: int = 0) -> dict:
    splits = jax.random.split(jax.random.key(seed), 10)
    return {
        "tokens": scatter_about(splits[0], (BATCH, ROWS, D), 1.0, 6.0, ((0, 4), (1, 8))),
        "w_x": scatter_about(splits[1], (D, H * P_SIZE), D ** -0.5, 0.125, ((0, 8),)),
        "w_bc": scatter_about(splits[2], (D, 2 * N), D ** -0.5, 0.125, ((0, 8),)),
        "w_dt": scatter_about(splits[3], (D, H), D ** -0.5, 0.125, ((0, 8),)),
        "dt_bias": jnp.clip(jax.random.uniform(splits[4], (H,), jnp.float32, -1.0, 0.5), -1.0, 0.5),
        "decay_rate": draw_decay_rate(jax.random.fold_in(splits[9], 71), 0),
        "gain": jnp.clip(1.0 + 0.1 * jax.random.normal(splits[6], (H * P_SIZE,), jnp.float32), 0.5, 1.5),
        "cotangent": scatter_about(splits[7], (BATCH, ROWS, H * P_SIZE), 0.001, 0.005859375, ((0, 4), (1, 8))),
        "counts": ragged(splits[8], GROUPS, TOTAL, CAP, 1).astype(jnp.int32),
    }


norm_floor = 1.0

def decay_weights(cumulative, dt_rows):
    length = cumulative.shape[0]
    causal = jnp.arange(length)[:, None] >= jnp.arange(length)[None, :]
    gap_log = cumulative.T[:, :, None] - cumulative.T[:, None, :]
    gap_log = jnp.where(causal[None, :, :], gap_log, -jnp.inf)
    return jnp.exp(gap_log) * dt_rows.T[:, None, :]

def stretch_state(inner, b_proj, dt_rows, a_neg):
    length = inner.shape[0]
    head_count = a_neg.shape[0]
    cumulative = jnp.cumsum(dt_rows * a_neg[None, :], axis=0)
    to_end = jnp.exp(cumulative[-1][None, :] - cumulative) * dt_rows
    scaled = (inner.astype(jnp.float32).reshape(length, head_count, -1) * to_end[:, :, None]).reshape(length, -1).astype(jnp.bfloat16)
    state_add = jnp.dot(scaled.T, b_proj, preferred_element_type=jnp.float32)
    return (jnp.exp(cumulative[-1]), state_add)

def stretch_outputs(inner, b_proj, c_proj, dt_rows, a_neg, state_in, gain, cot_rows, slot_used):
    length = inner.shape[0]
    head_count = a_neg.shape[0]
    head_size = inner.shape[1] // head_count
    cumulative = jnp.cumsum(dt_rows * a_neg[None, :], axis=0)
    weights = decay_weights(cumulative, dt_rows)
    gram_mat = jnp.dot(c_proj, b_proj.T, preferred_element_type=jnp.float32)
    mixing = (gram_mat[None, :, :] * weights).astype(jnp.bfloat16)
    inner_heads = inner.reshape(length, head_count, head_size)
    y_intra = jnp.einsum('hts,shp->thp', mixing.astype(jnp.float32), inner_heads.astype(jnp.float32))
    state_low = state_in.astype(jnp.bfloat16)
    growth = jnp.exp(cumulative)[:, :, None]
    y_inter = jnp.dot(c_proj, state_low.T, preferred_element_type=jnp.float32).reshape(length, head_count, head_size) * growth
    full = y_intra + y_inter
    radius = jnp.sqrt(lax.optimization_barrier(jnp.mean(full * full, axis=2, keepdims=True)) + norm_floor)
    gain_heads = gain.reshape(head_count, head_size)
    output = (full / radius * gain_heads * slot_used).reshape(length, -1).astype(jnp.bfloat16)
    grad_out = cot_rows.astype(jnp.float32).reshape(length, head_count, head_size) * gain_heads
    grad_full = (grad_out / radius - full * lax.optimization_barrier(jnp.sum(grad_out * full, axis=2, keepdims=True)) / (head_size * radius ** 3)) * slot_used
    grad_low = grad_full.astype(jnp.bfloat16)
    intersect = jnp.einsum('thp,shp->hts', grad_low.astype(jnp.float32), inner_heads.astype(jnp.float32))
    combined = lax.optimization_barrier(jnp.sum(intersect * weights, axis=0)).astype(jnp.bfloat16)
    grad_intra = jnp.dot(combined, b_proj, preferred_element_type=jnp.float32)
    scaled_grad = (grad_full * growth).reshape(length, -1).astype(jnp.bfloat16)
    grad_inter = jnp.dot(scaled_grad, state_low, preferred_element_type=jnp.float32)
    return (output, (grad_intra + grad_inter).astype(jnp.bfloat16))

def reference(tokens, w_x, w_bc, w_dt, dt_bias, decay_rate, gain, cotangent, counts):
    batch = tokens.shape[0]
    slot_total = tokens.shape[1] // L
    state_size = w_bc.shape[1] // 2
    head_count = decay_rate.shape[0]
    a_neg = -decay_rate
    token_blocks = tokens.reshape(batch, slot_total, L, -1).transpose(1, 0, 2, 3)
    cotangent_blocks = cotangent.reshape(batch, slot_total, L, -1).transpose(1, 0, 2, 3)
    slot_ids = jnp.arange(slot_total).astype(jnp.int32)
    filled = counts[slot_ids // CAP]
    slot_used = (slot_ids % CAP < filled).astype(jnp.float32)

    def advance(running, stretch_data):
        states, gradient = running
        token_rows, cot_rows, used = stretch_data
        inner = jnp.dot(token_rows, w_x, preferred_element_type=jnp.float32).astype(jnp.bfloat16)
        bc_raw = jnp.dot(token_rows, w_bc, preferred_element_type=jnp.float32)
        b_proj = bc_raw[:, :, :state_size].astype(jnp.bfloat16)
        c_proj = bc_raw[:, :, state_size:].astype(jnp.bfloat16)
        dt_rows = jax.nn.softplus(jnp.dot(token_rows, w_dt, preferred_element_type=jnp.float32) + dt_bias) * used
        decays, state_add = jax.vmap(stretch_state, in_axes=(0, 0, 0, None))(inner, b_proj, dt_rows, a_neg)
        output, grad_rows = jax.vmap(stretch_outputs, in_axes=(0, 0, 0, 0, None, 0, None, 0, None))(inner, b_proj, c_proj, dt_rows, a_neg, states, gain, cot_rows, used)
        gradient = gradient + jnp.einsum('btd,btn->dn', token_rows.astype(jnp.float32), grad_rows.astype(jnp.float32))
        states = (states.reshape(batch, head_count, -1) * decays[:, :, None]).reshape(states.shape) + state_add
        return ((states, gradient), output)
    starting = (jnp.zeros((batch, w_x.shape[1], state_size), jnp.float32), jnp.zeros((tokens.shape[2], state_size), jnp.float32))
    (unused, gradient), outputs = lax.scan(advance, starting, (token_blocks, cotangent_blocks, slot_used))
    ssm_output = outputs.transpose(1, 0, 2, 3).reshape(batch, tokens.shape[1], -1)
    return (ssm_output, gradient)
```

```python
import functools

import jax
import jax.numpy as jnp
from jax import lax
from jax.experimental import pallas as pl
from jax.experimental.pallas import tpu as pltpu
from jax.sharding import PartitionSpec as P

L = 256
LANES = 128
MESH = pl.DeviceIdType.MESH
VMEM_LIMIT = 60 * 1024 * 1024

norm_floor = 1.0


def greet(partners):
    barrier = pltpu.get_barrier_semaphore()
    for partner in partners:
        pl.semaphore_signal(barrier, inc=1, device_id=partner, device_id_type=MESH)
    pl.semaphore_wait(barrier, len(partners))


def wait_bytes(view, sem):
    pltpu.make_async_copy(view, view, sem).wait()


def project_kernel(
    seq_size, stages, tok_ref, wm_ref, we_ref, inner_ref, ext_ref,
    buf_e, buf_m, local_sem, send_sem, ring_sem, side_sem, pair_sem,
):
    dp, seq = lax.axis_index("dp"), lax.axis_index("seq")
    chips = seq_size // 2
    reach = chips // 2
    chip, core = seq // 2, seq % 2
    part = wm_ref.shape[0]
    half = (dp + dp // 2) % 2
    right = (dp, lax.rem(chip + 1, chips) * 2 + core)
    left = (dp, lax.rem(chip + chips - 1, chips) * 2 + core)
    side = (
        (dp + 1 - 2 * (dp % 2), seq),
        (dp + 2 - 4 * ((dp // 2) % 2), seq),
    )
    sibling = (dp, seq + 1 - 2 * core)

    def rows(offset):
        owner = lax.rem(chip + offset + chips, chips) * 2 + core
        return pl.ds(pl.multiple_of(owner * part, 16), part)

    def chunk(stage, slot, offset):
        if stage == 0:
            return buf_e.at[slot, rows(offset), :]
        return buf_m.at[slot * (stages - 1) + stage - 1, rows(offset), :]

    def sample(stage, slots, count):
        buf = buf_e if stage == 0 else buf_m
        return buf.at[pl.ds(0, slots), pl.ds(0, count * part), :]

    def send(stage, slot, offset, target, sem):
        view = chunk(stage, slot, offset)
        pltpu.make_async_remote_copy(
            src_ref=view, dst_ref=view, send_sem=send_sem.at[min(stage, 1)], recv_sem=sem,
            device_id=target, device_id_type=MESH,
        ).start()

    wide = buf_m.shape[2]
    slim = buf_e.shape[2]
    for stage in range(stages):
        for slot in range(4):
            if stage == 0:
                source = we_ref.at[:, pl.ds(slot * slim, slim)]
            else:
                source = wm_ref.at[:, pl.ds((slot * (stages - 1) + stage - 1) * wide, wide)]
            pltpu.make_async_copy(source, chunk(stage, slot, 0), local_sem.at[stage]).start()
    greet((right, left, sibling) + side)

    def quarters(direction, distance):
        return (0, 1) if distance < reach else (direction,)

    def own(stage):
        wait_bytes(sample(stage, 4, 1), local_sem.at[stage])
        for direction, target in ((0, right), (1, left)):
            for quarter in quarters(direction, 1):
                send(stage, half * 2 + quarter, 0, target, ring_sem.at[direction, stage, 0])
        for slot in range(4):
            send(stage, slot, 0, sibling, pair_sem.at[stage])

    def ring(stage, distance):
        for direction, target in ((0, right), (1, left)):
            got = quarters(direction, distance)
            offset = -distance if direction == 0 else distance
            wait_bytes(sample(stage, len(got), 1), ring_sem.at[direction, stage, distance - 1])
            if distance < reach:
                for quarter in quarters(direction, distance + 1):
                    send(
                        stage, half * 2 + quarter, offset, target,
                        ring_sem.at[direction, stage, distance],
                    )
            for quarter in got:
                send(stage, half * 2 + quarter, offset, side[quarter], side_sem.at[stage])
            for quarter in got:
                send(stage, half * 2 + quarter, offset, sibling, pair_sem.at[stage])

    def cross(stage):
        wait_bytes(sample(stage, 2, chips - 1), side_sem.at[stage])
        for offset in range(1, chips):
            for quarter in range(2):
                send(stage, (1 - half) * 2 + quarter, offset, sibling, pair_sem.at[stage])

    def multiply(stage):
        wait_bytes(sample(stage, 4, chips), pair_sem.at[stage])

        @pl.loop(0, 4)
        def _(slot):
            if stage == 0:
                ext_ref[:, pl.ds(pl.multiple_of(slot * slim, slim), slim)] = jnp.dot(
                    tok_ref[...], buf_e[slot], preferred_element_type=jnp.float32
                )
            else:
                index = slot * (stages - 1) + stage - 1
                inner_ref[:, pl.ds(pl.multiple_of(index * wide, wide), wide)] = jnp.dot(
                    tok_ref[...], buf_m[index], preferred_element_type=jnp.float32
                ).astype(jnp.bfloat16)

    tasks = []
    for stage in range(stages):
        for distance in range(1, reach + 1):
            tasks.append((stage * reach + distance, "ring", stage, distance))
        tasks.append((stage * reach + reach + 1.5, "cross", stage, 0))
        tasks.append((stage * reach + reach + 3.2, "multiply", stage, 0))
    own(0)
    own(1)
    for _, kind, stage, distance in sorted(tasks):
        if kind == "ring":
            ring(stage, distance)
            if distance == 1 and stage + 2 < stages:
                own(stage + 2)
        elif kind == "cross":
            cross(stage)
        else:
            multiply(stage)
    wait_bytes(sample(0, 4, seq_size - 1), send_sem.at[0])
    wait_bytes(sample(1, 4 * (stages - 1), seq_size - 1), send_sem.at[1])


def project(seq_tokens, w_main, w_ext, seq_size):
    total, depth = seq_tokens.shape
    width = w_main.shape[1]
    stages = 4
    wide = width // (4 * (stages - 1))
    slim = w_ext.shape[1] // 4
    reach = seq_size // 4
    vmem = pl.BlockSpec(memory_space=pltpu.VMEM)
    hbm = pl.BlockSpec(memory_space=pl.ANY)
    return pl.pallas_call(
        functools.partial(project_kernel, seq_size, stages),
        out_shape=(
            jax.ShapeDtypeStruct((total, width), jnp.bfloat16),
            jax.ShapeDtypeStruct((total, 4 * slim), jnp.float32),
        ),
        in_specs=[vmem, hbm, hbm],
        out_specs=(vmem, vmem),
        scratch_shapes=[
            pltpu.VMEM((4, depth, slim), jnp.bfloat16),
            pltpu.VMEM((4 * (stages - 1), depth, wide), jnp.bfloat16),
            pltpu.SemaphoreType.DMA((stages,)),
            pltpu.SemaphoreType.DMA((2,)),
            pltpu.SemaphoreType.DMA((2, stages, reach)),
            pltpu.SemaphoreType.DMA((stages,)),
            pltpu.SemaphoreType.DMA((stages,)),
        ],
        compiler_params=pltpu.CompilerParams(
            collective_id=0, has_side_effects=True, vmem_limit_bytes=VMEM_LIMIT
        ),
        name="project",
    )(seq_tokens, w_main, w_ext)


def others(axis_size, me):
    return [lax.rem(me + step, axis_size) for step in range(1, axis_size)]


def entering_kernel(
    seq_size, add_ref, decay_ref, enter_ref, adds, decays, back, local_sem, send_sem, recv_sem
):
    dp, seq = lax.axis_index("dp"), lax.axis_index("seq")
    width = adds.shape[2]

    def columns(index):
        return pl.ds(pl.multiple_of(index * width, LANES), width)

    peers = others(seq_size, seq)
    own = (
        pltpu.make_async_copy(add_ref.at[:, columns(seq)], adds.at[seq], local_sem.at[0]),
        pltpu.make_async_copy(decay_ref.at[:, columns(seq)], decays.at[seq], local_sem.at[1]),
    )
    for copy in own:
        copy.start()
    greet([(dp, peer) for peer in peers])
    copies = []
    for step, peer in enumerate(peers):
        for kind, (source, target) in enumerate(((decay_ref, decays), (add_ref, adds))):
            copy = pltpu.make_async_remote_copy(
                src_ref=source.at[:, columns(peer)], dst_ref=target.at[seq],
                send_sem=send_sem.at[kind, step], recv_sem=recv_sem.at[kind, step],
                device_id=(dp, peer), device_id_type=MESH,
            )
            copy.start()
            copies.append(copy)
    for copy in copies:
        copy.wait()
    for copy in own:
        copy.wait()
    running = jnp.zeros(adds.shape[1:], jnp.float32)
    for index in range(seq_size):
        back[index] = running.astype(jnp.bfloat16)
        if index + 1 < seq_size:
            running = running * decays[index][0:1, :] + adds[index].astype(jnp.float32)
    mine = pltpu.make_async_copy(back.at[seq], enter_ref.at[:, columns(seq)], local_sem.at[2])
    mine.start()
    copies = []
    for step, peer in enumerate(peers):
        copy = pltpu.make_async_remote_copy(
            src_ref=back.at[peer], dst_ref=enter_ref.at[:, columns(seq)],
            send_sem=send_sem.at[2, step], recv_sem=recv_sem.at[2, step],
            device_id=(dp, peer), device_id_type=MESH,
        )
        copy.start()
        copies.append(copy)
    for copy in copies:
        copy.wait()
    mine.wait()


def entering(addition, decay, seq_size):
    state_size, width = addition.shape
    blocks = -(-width // LANES)
    each = -(-blocks // seq_size) * LANES
    padding = each * seq_size - width
    if padding:
        addition = jnp.pad(addition, ((0, 0), (0, padding)))
        decay = jnp.pad(decay, ((0, 0), (0, padding)))
    hbm = pl.BlockSpec(memory_space=pl.ANY)
    vmem = pl.BlockSpec(memory_space=pltpu.VMEM)
    result = pl.pallas_call(
        functools.partial(entering_kernel, seq_size),
        out_shape=jax.ShapeDtypeStruct((state_size, each * seq_size), jnp.bfloat16),
        in_specs=[hbm, hbm],
        out_specs=hbm,
        scratch_shapes=[
            pltpu.VMEM((seq_size, state_size, each), jnp.bfloat16),
            pltpu.VMEM((seq_size, decay.shape[0], each), jnp.float32),
            pltpu.VMEM((seq_size, state_size, each), jnp.bfloat16),
            pltpu.SemaphoreType.DMA((3,)),
            pltpu.SemaphoreType.DMA((3, seq_size)),
            pltpu.SemaphoreType.DMA((3, seq_size)),
        ],
        compiler_params=pltpu.CompilerParams(
            collective_id=1, has_side_effects=True, vmem_limit_bytes=VMEM_LIMIT
        ),
        name="entering",
    )(addition, decay)
    return result[:, :width]


def reduce_kernel(
    seq_size, dp_size, part_ref, out_ref, landed, total, across, local_sem, send_sem, recv_sem,
    dp_send_sem, dp_recv_sem,
):
    dp, seq = lax.axis_index("dp"), lax.axis_index("seq")
    height = out_ref.shape[0]

    def rows(index):
        return pl.ds(pl.multiple_of(index * height, 16), height)

    peers = others(seq_size, seq)
    fellows = others(dp_size, dp)
    own = pltpu.make_async_copy(part_ref.at[rows(seq), :], landed.at[0], local_sem)
    own.start()
    greet([(dp, peer) for peer in peers] + [(fellow, seq) for fellow in fellows])
    copies = []
    for step, peer in enumerate(peers):
        copy = pltpu.make_async_remote_copy(
            src_ref=part_ref.at[rows(peer), :], dst_ref=landed.at[step + 1],
            send_sem=send_sem.at[step], recv_sem=recv_sem.at[step],
            device_id=(dp, peer), device_id_type=MESH,
        )
        copy.start()
        copies.append(copy)
    own.wait()
    for copy in copies:
        copy.wait()
    mine = landed[0].astype(jnp.float32)
    for step in range(1, seq_size):
        mine = mine + landed[step].astype(jnp.float32)
    total[...] = mine.astype(jnp.bfloat16)
    copies = []
    for step, fellow in enumerate(fellows):
        copy = pltpu.make_async_remote_copy(
            src_ref=total, dst_ref=across.at[step],
            send_sem=dp_send_sem.at[step], recv_sem=dp_recv_sem.at[step],
            device_id=(fellow, seq), device_id_type=MESH,
        )
        copy.start()
        copies.append(copy)
    for copy in copies:
        copy.wait()
    mine = total[...].astype(jnp.float32)
    for step in range(dp_size - 1):
        mine = mine + across[step].astype(jnp.float32)
    out_ref[...] = mine


def reduce_rows(partial, seq_size, dp_size):
    height = partial.shape[0] // seq_size
    width = partial.shape[1]
    hbm = pl.BlockSpec(memory_space=pl.ANY)
    vmem = pl.BlockSpec(memory_space=pltpu.VMEM)
    return pl.pallas_call(
        functools.partial(reduce_kernel, seq_size, dp_size),
        out_shape=jax.ShapeDtypeStruct((height, width), jnp.float32),
        in_specs=[hbm],
        out_specs=vmem,
        scratch_shapes=[
            pltpu.VMEM((seq_size, height, width), jnp.bfloat16),
            pltpu.VMEM((height, width), jnp.bfloat16),
            pltpu.VMEM((dp_size - 1, height, width), jnp.bfloat16),
            pltpu.SemaphoreType.DMA,
            pltpu.SemaphoreType.DMA((seq_size - 1,)),
            pltpu.SemaphoreType.DMA((seq_size - 1,)),
            pltpu.SemaphoreType.DMA((dp_size - 1,)),
            pltpu.SemaphoreType.DMA((dp_size - 1,)),
        ],
        compiler_params=pltpu.CompilerParams(
            collective_id=2, has_side_effects=True, vmem_limit_bytes=VMEM_LIMIT
        ),
        name="reduce_rows",
    )(partial)


def decay_weights(cumulative, dt_rows):
    length = cumulative.shape[0]
    causal = jnp.arange(length)[:, None] >= jnp.arange(length)[None, :]
    gap_log = cumulative.T[:, :, None] - cumulative.T[:, None, :]
    gap_log = jnp.where(causal[None, :, :], gap_log, -jnp.inf)
    return jnp.exp(gap_log) * dt_rows.T[:, None, :]


def stretch_state(inner, b_proj, cumulative, dt_rows, head_size):
    to_end = jnp.exp(cumulative[-1][None, :] - cumulative) * dt_rows
    scaled = (inner * jnp.repeat(to_end, head_size, axis=1)).astype(jnp.bfloat16)
    return jnp.dot(b_proj.T, scaled, preferred_element_type=jnp.float32)


def stretch_outputs(inner, b_proj, c_proj, cumulative, dt_rows, state_low, gain, cot_rows, used):
    length = inner.shape[0]
    head_count = cumulative.shape[1]
    head_size = inner.shape[1] // head_count
    weights = decay_weights(cumulative, dt_rows)
    gram_mat = jnp.dot(c_proj, b_proj.T, preferred_element_type=jnp.float32)
    mixing = (gram_mat[None, :, :] * weights).astype(jnp.bfloat16)
    inner_heads = inner.reshape(length, head_count, head_size)
    y_intra = jnp.einsum("hts,shp->thp", mixing, inner_heads, preferred_element_type=jnp.float32)
    growth = jnp.exp(cumulative)[:, :, None]
    y_inter = (
        jnp.dot(c_proj, state_low, preferred_element_type=jnp.float32).reshape(
            length, head_count, head_size
        )
        * growth
    )
    full = y_intra + y_inter
    radius = jnp.sqrt(jnp.mean(full * full, axis=2, keepdims=True) + norm_floor)
    gain_heads = gain.reshape(head_count, head_size)
    output = (full / radius * gain_heads * used).reshape(length, -1).astype(jnp.bfloat16)
    grad_out = cot_rows.reshape(length, head_count, head_size) * gain_heads
    grad_full = (
        grad_out / radius
        - full * jnp.sum(grad_out * full, axis=2, keepdims=True) / (head_size * radius**3)
    ) * used
    grad_low = grad_full.astype(jnp.bfloat16)
    intersect = jnp.einsum(
        "thp,shp->hts", grad_low, inner_heads, preferred_element_type=jnp.float32
    )
    combined = jnp.sum(intersect * weights, axis=0).astype(jnp.bfloat16)
    grad_intra = jnp.dot(combined, b_proj, preferred_element_type=jnp.float32)
    scaled_grad = (grad_full * growth).reshape(length, -1).astype(jnp.bfloat16)
    grad_inter = jnp.dot(scaled_grad, state_low.T, preferred_element_type=jnp.float32)
    return (output, (grad_intra + grad_inter).astype(jnp.bfloat16))


def body(dp_size, seq_size, tokens, w_x, w_bc, w_dt, dt_bias, decay_rate, gain, cotangent, counts):
    seq_tokens = tokens[0]
    cot_rows = cotangent[0]
    row_total = seq_tokens.shape[0]
    slot_count = row_total // L
    state_size = w_bc.shape[1] // 2
    head_count = decay_rate.shape[0]
    head_size = w_x.shape[1] // head_count
    group_index = lax.axis_index("seq")
    filled = jnp.sum(jnp.where(jnp.arange(counts.shape[0]) == group_index, counts, 0))
    slot_used = (jnp.arange(slot_count) < filled).astype(jnp.float32)
    ext_width = w_bc.shape[1] + w_dt.shape[1]
    ext_pad = -ext_width % (4 * LANES)
    w_ext = jnp.concatenate([w_bc, w_dt, jnp.zeros((w_dt.shape[0], ext_pad), w_dt.dtype)], axis=1)
    inner, ext = project(seq_tokens, w_x, w_ext, seq_size)
    b_proj = ext[:, :state_size].astype(jnp.bfloat16)
    c_proj = ext[:, state_size : 2 * state_size].astype(jnp.bfloat16)
    dt_raw = ext[:, 2 * state_size : 2 * state_size + head_count]
    dt_blocks = (
        jax.nn.softplus(dt_raw + dt_bias).reshape(slot_count, L, head_count)
        * slot_used[:, None, None]
    )
    cumulative = jnp.cumsum(dt_blocks * -decay_rate, axis=1)
    inner_blocks = inner.reshape(slot_count, L, -1)
    b_blocks = b_proj.reshape(slot_count, L, -1)
    c_blocks = c_proj.reshape(slot_count, L, -1)
    cot_blocks = cot_rows.reshape(slot_count, L, -1)
    running = jnp.zeros((state_size, inner.shape[1]), jnp.float32)
    passed = jnp.ones((1, inner.shape[1]), jnp.float32)
    priors = []
    for slot in range(slot_count):
        priors.append((running, passed))
        decay = jnp.repeat(jnp.exp(cumulative[slot, -1]), head_size)[None, :]
        addition = stretch_state(
            inner_blocks[slot], b_blocks[slot], cumulative[slot], dt_blocks[slot], head_size
        )
        running = running * decay + addition
        passed = passed * decay
    enter = entering(
        running.astype(jnp.bfloat16), jnp.broadcast_to(passed, (8, passed.shape[1])), seq_size
    )
    outputs, grads = [], []
    for slot in range(slot_count):
        prior, through = priors[slot]
        state_low = (enter.astype(jnp.float32) * through + prior).astype(jnp.bfloat16)
        output, grad = stretch_outputs(
            inner_blocks[slot], b_blocks[slot], c_blocks[slot], cumulative[slot], dt_blocks[slot],
            state_low, gain, cot_blocks[slot], slot_used[slot],
        )
        outputs.append(output)
        grads.append(grad)
    ssm_output = jnp.concatenate(outputs, axis=0)
    grad_c_rows = jnp.concatenate(grads, axis=0)
    partial = jnp.dot(seq_tokens.T, grad_c_rows, preferred_element_type=jnp.float32)
    gradient = reduce_rows(partial.astype(jnp.bfloat16), seq_size, dp_size)
    return (ssm_output[None], gradient)


def solution(mesh):
    return jax.shard_map(
        functools.partial(body, mesh.shape["dp"], mesh.shape["seq"]),
        mesh=mesh,
        in_specs=(
            P("dp", "seq", None),
            P("seq", None),
            P("seq", None),
            P("seq", None),
            P(),
            P(),
            P(),
            P("dp", "seq", None),
            P(),
        ),
        out_specs=(P("dp", "seq", None), P("seq", None)),
        check_vma=False,
    )
```

```python
import functools

import jax
import jax.numpy as jnp
from jax import lax
from jax.experimental import pallas as pl
from jax.experimental.pallas import tpu as pltpu
from jax.sharding import PartitionSpec as P

L = 256
LANES = 128
MESH = pl.DeviceIdType.MESH
VMEM_LIMIT = 60 * 1024 * 1024

norm_floor = 1.0


def greet(partners):
    barrier = pltpu.get_barrier_semaphore()
    for partner in partners:
        pl.semaphore_signal(barrier, inc=1, device_id=partner, device_id_type=MESH)
    pl.semaphore_wait(barrier, len(partners))


def wait_bytes(view, sem):
    pltpu.make_async_copy(view, view, sem).wait()


def project_kernel(
    seq_size, stages, tok_ref, wm_ref, we_ref, inner_ref, ext_ref,
    buf_e, buf_m, local_sem, send_sem, ring_sem, side_sem, pair_sem,
):
    dp, seq = lax.axis_index("dp"), lax.axis_index("seq")
    chips = seq_size // 2
    reach = chips // 2
    chip, core = seq // 2, seq % 2
    part = wm_ref.shape[0]
    half = (dp + dp // 2) % 2
    right = (dp, lax.rem(chip + 1, chips) * 2 + core)
    left = (dp, lax.rem(chip + chips - 1, chips) * 2 + core)
    side = (
        (dp + 1 - 2 * (dp % 2), seq),
        (dp + 2 - 4 * ((dp // 2) % 2), seq),
    )
    sibling = (dp, seq + 1 - 2 * core)

    def rows(offset):
        owner = lax.rem(chip + offset + chips, chips) * 2 + core
        return pl.ds(pl.multiple_of(owner * part, 16), part)

    def chunk(stage, slot, offset):
        if stage == 0:
            return buf_e.at[slot, rows(offset), :]
        return buf_m.at[slot * (stages - 1) + stage - 1, rows(offset), :]

    def sample(stage, slots, count):
        buf = buf_e if stage == 0 else buf_m
        return buf.at[pl.ds(0, slots), pl.ds(0, count * part), :]

    def send(stage, slot, offset, target, sem):
        view = chunk(stage, slot, offset)
        pltpu.make_async_remote_copy(
            src_ref=view, dst_ref=view, send_sem=send_sem.at[min(stage, 1)], recv_sem=sem,
            device_id=target, device_id_type=MESH,
        ).start()

    wide = buf_m.shape[2]
    slim = buf_e.shape[2]
    for stage in range(stages):
        for slot in range(4):
            if stage == 0:
                source = we_ref.at[:, pl.ds(slot * slim, slim)]
            else:
                source = wm_ref.at[:, pl.ds((slot * (stages - 1) + stage - 1) * wide, wide)]
            pltpu.make_async_copy(source, chunk(stage, slot, 0), local_sem.at[stage]).start()
    greet((right, left, sibling) + side)

    def quarters(direction, distance):
        return (0, 1) if distance < reach else (direction,)

    def own(stage):
        wait_bytes(sample(stage, 4, 1), local_sem.at[stage])
        for direction, target in ((0, right), (1, left)):
            for quarter in quarters(direction, 1):
                send(stage, half * 2 + quarter, 0, target, ring_sem.at[direction, stage, 0])
        for slot in range(4):
            send(stage, slot, 0, sibling, pair_sem.at[stage])

    def ring(stage, distance):
        for direction, target in ((0, right), (1, left)):
            got = quarters(direction, distance)
            offset = -distance if direction == 0 else distance
            wait_bytes(sample(stage, len(got), 1), ring_sem.at[direction, stage, distance - 1])
            if distance < reach:
                for quarter in quarters(direction, distance + 1):
                    send(
                        stage, half * 2 + quarter, offset, target,
                        ring_sem.at[direction, stage, distance],
                    )
            for quarter in got:
                send(stage, half * 2 + quarter, offset, side[quarter], side_sem.at[stage])
            for quarter in got:
                send(stage, half * 2 + quarter, offset, sibling, pair_sem.at[stage])

    def cross(stage):
        wait_bytes(sample(stage, 2, chips - 1), side_sem.at[stage])
        for offset in range(1, chips):
            for quarter in range(2):
                send(stage, (1 - half) * 2 + quarter, offset, sibling, pair_sem.at[stage])

    def multiply(stage):
        wait_bytes(sample(stage, 4, chips), pair_sem.at[stage])

        @pl.loop(0, 4)
        def _(slot):
            if stage == 0:
                ext_ref[:, pl.ds(pl.multiple_of(slot * slim, slim), slim)] = jnp.dot(
                    tok_ref[...], buf_e[slot], preferred_element_type=jnp.float32
                )
            else:
                index = slot * (stages - 1) + stage - 1
                inner_ref[:, pl.ds(pl.multiple_of(index * wide, wide), wide)] = jnp.dot(
                    tok_ref[...], buf_m[index], preferred_element_type=jnp.float32
                ).astype(jnp.bfloat16)

    tasks = []
    for stage in range(stages):
        for distance in range(1, reach + 1):
            tasks.append((stage * reach + distance, "ring", stage, distance))
        tasks.append((stage * reach + reach + 1.5, "cross", stage, 0))
        tasks.append((stage * reach + reach + 3.2, "multiply", stage, 0))
    own(0)
    own(1)
    for _, kind, stage, distance in sorted(tasks):
        if kind == "ring":
            ring(stage, distance)
            if distance == 1 and stage + 2 < stages:
                own(stage + 2)
        elif kind == "cross":
            cross(stage)
        else:
            multiply(stage)
    wait_bytes(sample(0, 4, seq_size - 1), send_sem.at[0])
    wait_bytes(sample(1, 4 * (stages - 1), seq_size - 1), send_sem.at[1])


def project(seq_tokens, w_main, w_ext, seq_size):
    total, depth = seq_tokens.shape
    width = w_main.shape[1]
    stages = 4
    wide = width // (4 * (stages - 1))
    slim = w_ext.shape[1] // 4
    reach = seq_size // 4
    vmem = pl.BlockSpec(memory_space=pltpu.VMEM)
    hbm = pl.BlockSpec(memory_space=pl.ANY)
    return pl.pallas_call(
        functools.partial(project_kernel, seq_size, stages),
        out_shape=(
            jax.ShapeDtypeStruct((total, width), jnp.bfloat16),
            jax.ShapeDtypeStruct((total, 4 * slim), jnp.float32),
        ),
        in_specs=[vmem, hbm, hbm],
        out_specs=(vmem, vmem),
        scratch_shapes=[
            pltpu.VMEM((4, depth, slim), jnp.bfloat16),
            pltpu.VMEM((4 * (stages - 1), depth, wide), jnp.bfloat16),
            pltpu.SemaphoreType.DMA((stages,)),
            pltpu.SemaphoreType.DMA((2,)),
            pltpu.SemaphoreType.DMA((2, stages, reach)),
            pltpu.SemaphoreType.DMA((stages,)),
            pltpu.SemaphoreType.DMA((stages,)),
        ],
        compiler_params=pltpu.CompilerParams(
            collective_id=0, has_side_effects=True, vmem_limit_bytes=VMEM_LIMIT
        ),
        name="project",
    )(seq_tokens, w_main, w_ext)


def others(axis_size, me):
    return [lax.rem(me + step, axis_size) for step in range(1, axis_size)]


def entering_kernel(
    seq_size, add_ref, decay_ref, enter_ref, adds, decays, back, local_sem, send_sem, recv_sem
):
    dp, seq = lax.axis_index("dp"), lax.axis_index("seq")
    width = adds.shape[2]

    def columns(index):
        return pl.ds(pl.multiple_of(index * width, LANES), width)

    peers = others(seq_size, seq)
    own = (
        pltpu.make_async_copy(add_ref.at[:, columns(seq)], adds.at[seq], local_sem.at[0]),
        pltpu.make_async_copy(decay_ref.at[:, columns(seq)], decays.at[seq], local_sem.at[1]),
    )
    for copy in own:
        copy.start()
    greet([(dp, peer) for peer in peers])
    copies = []
    for step, peer in enumerate(peers):
        for kind, (source, target) in enumerate(((decay_ref, decays), (add_ref, adds))):
            copy = pltpu.make_async_remote_copy(
                src_ref=source.at[:, columns(peer)], dst_ref=target.at[seq],
                send_sem=send_sem.at[kind, step], recv_sem=recv_sem.at[kind, step],
                device_id=(dp, peer), device_id_type=MESH,
            )
            copy.start()
            copies.append(copy)
    for copy in copies:
        copy.wait()
    for copy in own:
        copy.wait()
    running = jnp.zeros(adds.shape[1:], jnp.float32)
    for index in range(seq_size):
        back[index] = running.astype(jnp.bfloat16)
        if index + 1 < seq_size:
            running = running * decays[index][0:1, :] + adds[index].astype(jnp.float32)
    mine = pltpu.make_async_copy(back.at[seq], enter_ref.at[:, columns(seq)], local_sem.at[2])
    mine.start()
    copies = []
    for step, peer in enumerate(peers):
        copy = pltpu.make_async_remote_copy(
            src_ref=back.at[peer], dst_ref=enter_ref.at[:, columns(seq)],
            send_sem=send_sem.at[2, step], recv_sem=recv_sem.at[2, step],
            device_id=(dp, peer), device_id_type=MESH,
        )
        copy.start()
        copies.append(copy)
    for copy in copies:
        copy.wait()
    mine.wait()


def entering(addition, decay, seq_size):
    state_size, width = addition.shape
    blocks = -(-width // LANES)
    each = -(-blocks // seq_size) * LANES
    padding = each * seq_size - width
    if padding:
        addition = jnp.pad(addition, ((0, 0), (0, padding)))
        decay = jnp.pad(decay, ((0, 0), (0, padding)))
    hbm = pl.BlockSpec(memory_space=pl.ANY)
    vmem = pl.BlockSpec(memory_space=pltpu.VMEM)
    result = pl.pallas_call(
        functools.partial(entering_kernel, seq_size),
        out_shape=jax.ShapeDtypeStruct((state_size, each * seq_size), jnp.bfloat16),
        in_specs=[hbm, hbm],
        out_specs=hbm,
        scratch_shapes=[
            pltpu.VMEM((seq_size, state_size, each), jnp.bfloat16),
            pltpu.VMEM((seq_size, decay.shape[0], each), jnp.float32),
            pltpu.VMEM((seq_size, state_size, each), jnp.bfloat16),
            pltpu.SemaphoreType.DMA((3,)),
            pltpu.SemaphoreType.DMA((3, seq_size)),
            pltpu.SemaphoreType.DMA((3, seq_size)),
        ],
        compiler_params=pltpu.CompilerParams(
            collective_id=1, has_side_effects=True, vmem_limit_bytes=VMEM_LIMIT
        ),
        name="entering",
    )(addition, decay)
    return result[:, :width]


def reduce_kernel(
    seq_size, dp_size, part_ref, out_ref, landed, total, across, local_sem, send_sem, recv_sem,
    dp_send_sem, dp_recv_sem,
):
    dp, seq = lax.axis_index("dp"), lax.axis_index("seq")
    height = out_ref.shape[0]

    def rows(index):
        return pl.ds(pl.multiple_of(index * height, 16), height)

    peers = others(seq_size, seq)
    fellows = others(dp_size, dp)
    own = pltpu.make_async_copy(part_ref.at[rows(seq), :], landed.at[0], local_sem)
    own.start()
    greet([(dp, peer) for peer in peers] + [(fellow, seq) for fellow in fellows])
    copies = []
    for step, peer in enumerate(peers):
        copy = pltpu.make_async_remote_copy(
            src_ref=part_ref.at[rows(peer), :], dst_ref=landed.at[step + 1],
            send_sem=send_sem.at[step], recv_sem=recv_sem.at[step],
            device_id=(dp, peer), device_id_type=MESH,
        )
        copy.start()
        copies.append(copy)
    own.wait()
    for copy in copies:
        copy.wait()
    mine = landed[0].astype(jnp.float32)
    for step in range(1, seq_size):
        mine = mine + landed[step].astype(jnp.float32)
    total[...] = mine.astype(jnp.bfloat16)
    copies = []
    for step, fellow in enumerate(fellows):
        copy = pltpu.make_async_remote_copy(
            src_ref=total, dst_ref=across.at[step],
            send_sem=dp_send_sem.at[step], recv_sem=dp_recv_sem.at[step],
            device_id=(fellow, seq), device_id_type=MESH,
        )
        copy.start()
        copies.append(copy)
    for copy in copies:
        copy.wait()
    mine = total[...].astype(jnp.float32)
    for step in range(dp_size - 1):
        mine = mine + across[step].astype(jnp.float32)
    out_ref[...] = mine


def reduce_rows(partial, seq_size, dp_size):
    height = partial.shape[0] // seq_size
    width = partial.shape[1]
    hbm = pl.BlockSpec(memory_space=pl.ANY)
    vmem = pl.BlockSpec(memory_space=pltpu.VMEM)
    return pl.pallas_call(
        functools.partial(reduce_kernel, seq_size, dp_size),
        out_shape=jax.ShapeDtypeStruct((height, width), jnp.float32),
        in_specs=[hbm],
        out_specs=vmem,
        scratch_shapes=[
            pltpu.VMEM((seq_size, height, width), jnp.bfloat16),
            pltpu.VMEM((height, width), jnp.bfloat16),
            pltpu.VMEM((dp_size - 1, height, width), jnp.bfloat16),
            pltpu.SemaphoreType.DMA,
            pltpu.SemaphoreType.DMA((seq_size - 1,)),
            pltpu.SemaphoreType.DMA((seq_size - 1,)),
            pltpu.SemaphoreType.DMA((dp_size - 1,)),
            pltpu.SemaphoreType.DMA((dp_size - 1,)),
        ],
        compiler_params=pltpu.CompilerParams(
            collective_id=2, has_side_effects=True, vmem_limit_bytes=VMEM_LIMIT
        ),
        name="reduce_rows",
    )(partial)


def stretch_state(inner, b_proj, cumulative, dt_rows, head_size):
    to_end = jnp.exp(cumulative[-1][None, :] - cumulative) * dt_rows
    scaled = (inner * jnp.repeat(to_end, head_size, axis=1)).astype(jnp.bfloat16)
    return jnp.dot(b_proj.T, scaled, preferred_element_type=jnp.float32)


def outputs_kernel(
    head_size, used_ref, b_ref, c_ref, inner_ref, cot_ref, cum_ref, cum_row_ref, dt_row_ref,
    state_ref, gain_ref, out_ref, grad_ref, gram, combined, carried,
):
    slot, pair = pl.program_id(0), pl.program_id(1)

    @pl.when(pair == 0)
    def _():
        gram[...] = lax.dot_general(
            c_ref[...], b_ref[...], (((1,), (1,)), ((), ())), preferred_element_type=jnp.float32
        )
        combined[...] = jnp.zeros_like(combined)
        carried[...] = jnp.zeros_like(carried)

    length, width = inner_ref.shape
    heads = width // head_size
    used = used_ref[slot]
    inner = inner_ref[...]
    state = state_ref[0]
    lane_head = lax.broadcasted_iota(jnp.int32, (length, width), 1) // head_size
    causal = lax.broadcasted_iota(jnp.int32, (length, length), 0) >= lax.broadcasted_iota(
        jnp.int32, (length, length), 1
    )

    def spread(columns):
        result = columns[0]
        for head in range(1, heads):
            result = jnp.where(lane_head == head, columns[head], result)
        return jnp.broadcast_to(result, (length, width))

    def head_sums(values):
        return spread([
            jnp.sum(jnp.where(lane_head == head, values, 0.0), axis=1, keepdims=True)
            for head in range(heads)
        ])

    weights = []
    intra = []
    for head in range(heads):
        gap = cum_ref[0, 0, :, head : head + 1] - cum_row_ref[0, 0, head : head + 1, :]
        weight = jnp.exp(jnp.where(causal, gap, -jnp.inf)) * dt_row_ref[0, 0, head : head + 1, :]
        weights.append(weight)
        mixing = (gram[...] * weight).astype(jnp.bfloat16)
        intra.append(jnp.dot(mixing, inner, preferred_element_type=jnp.float32))
    growth = spread([jnp.exp(cum_ref[0, 0, :, head : head + 1]) for head in range(heads)])
    full = spread(intra) + growth * jnp.dot(c_ref[...], state, preferred_element_type=jnp.float32)
    inverse = 1.0 / jnp.sqrt(head_sums(full * full) * (1.0 / head_size) + norm_floor)
    gain = gain_ref[...]
    out_ref[...] = (full * inverse * gain * used).astype(jnp.bfloat16)
    grad_out = cot_ref[...].astype(jnp.float32) * gain
    pull = head_sums(grad_out * full) * (1.0 / head_size)
    grad_full = (grad_out * inverse - full * pull * (inverse * inverse * inverse)) * used
    total = combined[...]
    for head in range(heads):
        grad_low = jnp.where(lane_head == head, grad_full, 0.0).astype(jnp.bfloat16)
        intersect = lax.dot_general(
            grad_low, inner, (((1,), (1,)), ((), ())), preferred_element_type=jnp.float32
        )
        total = total + intersect * weights[head]
    combined[...] = total
    carried[...] += lax.dot_general(
        (grad_full * growth).astype(jnp.bfloat16), state, (((1,), (1,)), ((), ())),
        preferred_element_type=jnp.float32,
    )

    @pl.when(pair == pl.num_programs(1) - 1)
    def _():
        grad_ref[...] = (
            carried[...]
            + jnp.dot(
                combined[...].astype(jnp.bfloat16), b_ref[...], preferred_element_type=jnp.float32
            )
        ).astype(jnp.bfloat16)


def stretch_outputs(inner, b_proj, c_proj, cumulative, dt_blocks, states, gain, cot_rows, used):
    slots, length, head_count = cumulative.shape
    width = inner.shape[1]
    head_size = width // head_count
    heads = LANES // head_size
    pairs = head_count // heads
    state_size = b_proj.shape[1]
    cum_rows = cumulative.transpose(0, 2, 1).reshape(slots, pairs, heads, length)
    dt_rows = dt_blocks.transpose(0, 2, 1).reshape(slots, pairs, heads, length)
    cum_columns = cumulative.reshape(slots, length, pairs, heads).transpose(0, 2, 1, 3)
    by_slot = pl.BlockSpec((length, state_size), lambda slot, pair: (slot, 0))
    by_pair = pl.BlockSpec((length, LANES), lambda slot, pair: (slot, pair))
    row_spec = pl.BlockSpec((1, 1, heads, length), lambda slot, pair: (slot, pair, 0, 0))
    return pl.pallas_call(
        functools.partial(outputs_kernel, head_size),
        grid=(slots, pairs),
        out_shape=(
            jax.ShapeDtypeStruct((slots * length, width), jnp.bfloat16),
            jax.ShapeDtypeStruct((slots * length, state_size), jnp.bfloat16),
        ),
        in_specs=[
            pl.BlockSpec(memory_space=pltpu.SMEM),
            by_slot,
            by_slot,
            by_pair,
            by_pair,
            pl.BlockSpec((1, 1, length, heads), lambda slot, pair: (slot, pair, 0, 0)),
            row_spec,
            row_spec,
            pl.BlockSpec((1, state_size, LANES), lambda slot, pair: (slot, 0, pair)),
            pl.BlockSpec((1, LANES), lambda slot, pair: (0, pair)),
        ],
        out_specs=(by_pair, by_slot),
        scratch_shapes=[
            pltpu.VMEM((length, length), jnp.float32),
            pltpu.VMEM((length, length), jnp.float32),
            pltpu.VMEM((length, state_size), jnp.float32),
        ],
        name="outputs",
    )(used, b_proj, c_proj, inner, cot_rows, cum_columns, cum_rows, dt_rows, states, gain[None, :])


def body(dp_size, seq_size, tokens, w_x, w_bc, w_dt, dt_bias, decay_rate, gain, cotangent, counts):
    seq_tokens = tokens[0]
    cot_rows = cotangent[0]
    row_total = seq_tokens.shape[0]
    slot_count = row_total // L
    state_size = w_bc.shape[1] // 2
    head_count = decay_rate.shape[0]
    head_size = w_x.shape[1] // head_count
    group_index = lax.axis_index("seq")
    filled = jnp.sum(jnp.where(jnp.arange(counts.shape[0]) == group_index, counts, 0))
    slot_used = (jnp.arange(slot_count) < filled).astype(jnp.float32)
    ext_width = w_bc.shape[1] + w_dt.shape[1]
    ext_pad = -ext_width % (4 * LANES)
    w_ext = jnp.concatenate([w_bc, w_dt, jnp.zeros((w_dt.shape[0], ext_pad), w_dt.dtype)], axis=1)
    inner, ext = project(seq_tokens, w_x, w_ext, seq_size)
    b_proj = ext[:, :state_size].astype(jnp.bfloat16)
    c_proj = ext[:, state_size : 2 * state_size].astype(jnp.bfloat16)
    dt_raw = ext[:, 2 * state_size : 2 * state_size + head_count]
    dt_blocks = (
        jax.nn.softplus(dt_raw + dt_bias).reshape(slot_count, L, head_count)
        * slot_used[:, None, None]
    )
    cumulative = jnp.cumsum(dt_blocks * -decay_rate, axis=1)
    inner_blocks = inner.reshape(slot_count, L, -1)
    b_blocks = b_proj.reshape(slot_count, L, -1)
    running = jnp.zeros((state_size, inner.shape[1]), jnp.float32)
    passed = jnp.ones((1, inner.shape[1]), jnp.float32)
    priors = []
    for slot in range(slot_count):
        priors.append((running, passed))
        decay = jnp.repeat(jnp.exp(cumulative[slot, -1]), head_size)[None, :]
        addition = stretch_state(
            inner_blocks[slot], b_blocks[slot], cumulative[slot], dt_blocks[slot], head_size
        )
        running = running * decay + addition
        passed = passed * decay
    enter = entering(
        running.astype(jnp.bfloat16), jnp.broadcast_to(passed, (8, passed.shape[1])), seq_size
    )
    states = jnp.stack([
        (enter.astype(jnp.float32) * through + prior).astype(jnp.bfloat16)
        for prior, through in priors
    ])
    ssm_output, grad_c_rows = stretch_outputs(
        inner, b_proj, c_proj, cumulative, dt_blocks, states, gain, cot_rows, slot_used
    )
    partial = jnp.dot(seq_tokens.T, grad_c_rows, preferred_element_type=jnp.float32)
    gradient = reduce_rows(partial.astype(jnp.bfloat16), seq_size, dp_size)
    return (ssm_output[None], gradient)


def solution(mesh):
    return jax.shard_map(
        functools.partial(body, mesh.shape["dp"], mesh.shape["seq"]),
        mesh=mesh,
        in_specs=(
            P("dp", "seq", None),
            P("seq", None),
            P("seq", None),
            P("seq", None),
            P(),
            P(),
            P(),
            P("dp", "seq", None),
            P(),
        ),
        out_specs=(P("dp", "seq", None), P("seq", None)),
        check_vma=False,
    )
```
